32 devices in a mesh: rows: 8 (over y, x, core), cols: 4 (over z).
Axes of the slice: x: 2, y: 2, z: 4, core: 2. Of those that a mesh axis runs over, the one named last changes fastest.
Arguments:
- inputs: bfloat16 [2, 6144, 2048], P(None, 'rows', 'cols'), may hold values from -6 to 6
- lengths: int32 [2, 4, 3], P(None, 'cols'), may hold values from 1 to 1024, 1536 in all within a row
- gain_attn: bfloat16 [2048], P('cols'), may hold values from 0.25 to 1.75
- w_query: bfloat16 [2048, 2048], P('cols', 'rows'), may hold values from -0.125 to 0.125
- key_weight: bfloat16 [2048, 256], P('cols'), may hold values from -0.125 to 0.125
- value_weight: bfloat16 [2048, 256], P('cols'), may hold values from -0.125 to 0.125
- w_out: bfloat16 [2048, 2048], P('rows', 'cols'), may hold values from -2 to 2
- gain_ffn: bfloat16 [2048], P('cols'), may hold values from 0.25 to 1.75
- w_gate: bfloat16 [2048, 5632], P('cols', 'rows'), may hold values from -0.125 to 0.125
- w_up: bfloat16 [2048, 5632], P('cols', 'rows'), may hold values from -0.125 to 0.125
- w_down: bfloat16 [5632, 2048], P('rows', 'cols'), may hold values from -0.078125 to 0.078125
- cotangent: bfloat16 [2, 6144, 2048], P(None, 'rows', 'cols'), may hold values from -6 to 6
Outputs:
- output: bfloat16 [2, 6144, 2048], P(None, 'rows', 'cols')
- input_grad: float32 [2, 6144, 2048], P(None, 'rows', 'cols')
- grad_gain_attn: float32 [2048], P('cols')
- grad_query: float32 [2048, 2048], P('cols', 'rows')
- grad_key: float32 [2048, 256], P('cols')
- grad_value: float32 [2048, 256], P('cols')
- grad_out: float32 [2048, 2048], P('rows', 'cols')
- grad_gain_ffn: float32 [2048], P('cols')
- grad_gate: float32 [2048, 5632], P('cols', 'rows')
- grad_up: float32 [2048, 5632], P('cols', 'rows')
- grad_down: float32 [5632, 2048], P('rows', 'cols')
The draws below stay inside these ranges and needn't reach their ends.
Inputs may be any that keep to these rules, and one draw needn't show every extreme that they name: Each row of 3 lengths sums to 1536; one length of each row is exactly 1024.
All inputs are finite; a program needn't handle non-finite values.
Results may differ from the reference program's by a relative error of at most 0.023.
Values may be sent and summed in bfloat16 or wider, within the bound.
A program may use at most 192 MiB of HBM per device.

```python
import math
import jax
import jax.numpy as jnp
import numpy as np
from jax import lax

MODEL_WIDTH = 2048
QUERY_HEADS = 32
KEY_VALUE_HEADS = 4
HEAD_SIZE = 64
FF = 5632
PACKED_TOKENS = 1536
NSEQ = 3
MB = 2
PACKED_BLOCKS = 4
TOKB = 6144
LONGEST = 1024
N_ROWS = 8


def block_scale(key, shape, shards, least, top_value):
    gain, own = 1.0, jax.random.fold_in(key, 6)
    for axis_at, blocks in shards:
        steps = jnp.exp(jax.random.uniform(jax.random.fold_in(own, axis_at), (blocks,), jnp.float32, least / len(shards), top_value / len(shards)))
        gain = gain * jnp.repeat(steps, shape[axis_at] // blocks).reshape([-1 if axis == axis_at else 1 for axis in range(len(shape))])
    return gain


def split_up(amount, total, most, lean):
    portions = [(1 << 20) // math.isqrt(standing ** lean) + 1 for standing in range(2, amount + 1)]
    spare, given = total - most - (amount - 1), [1] * (amount - 1)
    while spare > 0:
        free = [i for i in range(amount - 1) if given[i] < most]
        whole, budget = sum([portions[i] for i in free]), spare
        for i in free:
            more = min(most - given[i], max(1, budget * portions[i] // whole), spare)
            given[i] = given[i] + more
            spare = spare - more
    return np.array([most] + given)


def uneven_parts(key, amount, total, bound, slope):
    if amount == 2:
        one = jax.random.randint(key, (), max(1, total - bound), min(bound, total - 1) + 1)
        return jnp.stack([one, total - one])
    sizes = jnp.asarray(split_up(amount, total, bound, slope), jnp.int32)
    twos = (amount - 1) // 2
    giver, receiver = sizes[1:1 + 2 * twos:2], sizes[2:2 + 2 * twos:2]
    room = jnp.minimum(giver - 1, bound - receiver)
    moved = jax.random.randint(jax.random.fold_in(key, 1), (twos,), 0, 1 << 20) % (room + 1)
    sizes = sizes.at[1:1 + 2 * twos:2].set(giver - moved).at[2:2 + 2 * twos:2].set(receiver + moved)
    return sizes[jax.random.permutation(jax.random.fold_in(key, 2), amount)]


def normal_values(stream_key, dims, deviation, most, shards=(), held_as=jnp.bfloat16):
    entries = jax.random.normal(stream_key, dims, jnp.float32) * deviation
    if len(shards) > 0:
        entries = block_scale(stream_key, dims, shards, -0.22, 0.18) * entries
    return jnp.clip(entries, min=-most, max=most).astype(held_as)


def setup_inputs(seed: int = 0) -> dict:
    key_of = jax.random.split(jax.random.key(seed), 13)
    inputs = normal_values(key_of[0], (MB, TOKB, MODEL_WIDTH), 1.0, 6.0, ((1, 8), (2, 4)))
    lengths = jax.vmap(lambda own: uneven_parts(own, NSEQ, PACKED_TOKENS, LONGEST, 2))(jax.random.split(key_of[1], MB * PACKED_BLOCKS)).reshape((MB, PACKED_BLOCKS, NSEQ)).astype(jnp.int32)
    gain_attn = jnp.clip(1.0 + 0.15 * jax.random.normal(key_of[2], (MODEL_WIDTH,), jnp.float32), 0.25, 1.75).astype(jnp.bfloat16)
    w_query = normal_values(key_of[3], (MODEL_WIDTH, QUERY_HEADS * HEAD_SIZE), MODEL_WIDTH ** -0.5, 0.125, ((0, 4), (1, 8)))
    key_weight = normal_values(key_of[4], (MODEL_WIDTH, KEY_VALUE_HEADS * HEAD_SIZE), MODEL_WIDTH ** -0.5, 0.125, ((0, 4),))
    value_weight = normal_values(key_of[5], (MODEL_WIDTH, KEY_VALUE_HEADS * HEAD_SIZE), MODEL_WIDTH ** -0.5, 0.125, ((0, 4),))
    w_out = normal_values(key_of[6], (QUERY_HEADS * HEAD_SIZE, MODEL_WIDTH), (max(QUERY_HEADS * HEAD_SIZE // 256, 2)) ** -0.5, 2.0, ((0, 8), (1, 4)))
    gain_ffn = jnp.clip(1.0 + 0.15 * jax.random.normal(key_of[7], (MODEL_WIDTH,), jnp.float32), 0.25, 1.75).astype(jnp.bfloat16)
    w_gate = normal_values(key_of[8], (MODEL_WIDTH, FF), MODEL_WIDTH ** -0.5, 0.125, ((0, 4), (1, 8)))
    w_up = normal_values(key_of[9], (MODEL_WIDTH, FF), MODEL_WIDTH ** -0.5, 0.125, ((0, 4), (1, 8)))
    w_down = normal_values(key_of[10], (FF, MODEL_WIDTH), FF ** -0.5, 0.078125, ((0, 8), (1, 4)))
    cotangent = normal_values(key_of[11], (MB, TOKB, MODEL_WIDTH), 1.0, 6.0, ((1, 8), (2, 4)))
    return {"inputs": inputs, "lengths": lengths, "gain_attn": gain_attn, "w_query": w_query, "key_weight": key_weight, "value_weight": value_weight, "w_out": w_out, "gain_ffn": gain_ffn, "w_gate": w_gate, "w_up": w_up, "w_down": w_down, "cotangent": cotangent}


eps_norm = 1e-05
rope_base = 10000.0
highest_precision = lax.Precision.HIGHEST

@jax.custom_vjp
def low(v):
    return lax.optimization_barrier(v.astype(jnp.bfloat16)).astype(jnp.float32)

@jax.custom_vjp
def low_back(v):
    return v

def low_keep(v):
    return (low(v), None)

def low_pass(kept, grad):
    return (grad,)

def back_keep(v):
    return (v, None)

def back_low(kept, grad):
    return (low(grad),)
low.defvjp(low_keep, low_pass)
low_back.defvjp(back_keep, back_low)

def slab_layout(counts, extent):
    counts = counts.astype(jnp.int32)
    bounds = jnp.cumsum(counts).astype(jnp.int32)
    places = jnp.arange(extent, dtype=jnp.int32)
    passed = (places[:, None] >= bounds[None, :]).astype(jnp.int32)
    segment = lax.optimization_barrier(jnp.sum(passed, axis=1)).astype(jnp.int32)
    offsets = lax.optimization_barrier(jnp.sum(passed * counts[None, :], axis=1)).astype(jnp.int32)
    return (segment, places - offsets)

def rope_tables(positions, head_dim):
    half_dim = head_dim // 2
    frequency = jnp.exp(-jnp.log(rope_base) * (2.0 * jnp.arange(half_dim, dtype=jnp.float32) / head_dim))
    angles = positions.astype(jnp.float32)[:, None] * frequency[None, :]
    return (jnp.cos(angles)[:, None, :], jnp.sin(angles)[:, None, :])

def rotate(tensor, cosine_table, sine_table):
    half_dim = tensor.shape[-1] // 2
    first_half = tensor[..., :half_dim]
    second_half = tensor[..., half_dim:]
    return jnp.concatenate([first_half * cosine_table - second_half * sine_table, second_half * cosine_table + first_half * sine_table], axis=-1)

def rms_norm(values_in, gain_row):
    return values_in * lax.rsqrt(lax.optimization_barrier(jnp.mean(values_in * values_in, axis=-1, keepdims=True)) + eps_norm) * gain_row

def slab_attention(pieces):
    queries, key_head_rows, value_head_rows, counts = pieces
    segment, positions = slab_layout(counts, PACKED_TOKENS)
    cosine_table, sine_table = rope_tables(positions, HEAD_SIZE)
    heads_per_replica = QUERY_HEADS // N_ROWS
    replicated_heads = jnp.arange(N_ROWS, dtype=jnp.int32) * heads_per_replica // (QUERY_HEADS // KEY_VALUE_HEADS)
    key_copies = low(rotate(low_back(key_head_rows[:, replicated_heads, :]), cosine_table, sine_table))
    value_copies = low(low_back(value_head_rows[:, replicated_heads, :]))
    query_rot = low(rotate(low_back(queries), cosine_table, sine_table))
    places = jnp.arange(PACKED_TOKENS, dtype=jnp.int32)
    allowed = (segment[:, None] == segment[None, :]) & (places[None, :] <= places[:, None])

    def one_copy(group_pieces):
        query_group, key_one, value_one = group_pieces
        scores = low_back(jnp.einsum('qhd,kd->hqk', query_group, key_one, precision=highest_precision) * HEAD_SIZE ** (-0.5))
        scores = jnp.where(allowed[None], scores, -1e+30)
        probs_all = jax.nn.softmax(scores, axis=-1)
        return jnp.einsum('hqk,kd->qhd', low(probs_all), value_one, precision=highest_precision)
    query_groups = jnp.transpose(query_rot.reshape(PACKED_TOKENS, N_ROWS, heads_per_replica, HEAD_SIZE), (1, 0, 2, 3))
    mixed_out = lax.map(jax.checkpoint(one_copy), (query_groups, jnp.transpose(key_copies, (1, 0, 2)), jnp.transpose(value_copies, (1, 0, 2))))
    return jnp.transpose(mixed_out, (1, 0, 2, 3)).reshape(PACKED_TOKENS, QUERY_HEADS * HEAD_SIZE)

def decoder_layer(pieces, weights):
    block_in, counts = pieces
    gain_attn, w_query, key_weight, value_weight, w_out, gain_ffn, w_gate, w_up, w_down = weights
    normed_input = low(rms_norm(block_in, gain_attn))
    queries = jnp.dot(normed_input, w_query, precision=highest_precision).reshape(PACKED_BLOCKS, PACKED_TOKENS, QUERY_HEADS, HEAD_SIZE)
    key_head_rows = jnp.dot(normed_input, key_weight, precision=highest_precision).reshape(PACKED_BLOCKS, PACKED_TOKENS, KEY_VALUE_HEADS, HEAD_SIZE)
    value_head_rows = jnp.dot(normed_input, value_weight, precision=highest_precision).reshape(PACKED_BLOCKS, PACKED_TOKENS, KEY_VALUE_HEADS, HEAD_SIZE)
    mixed_out = lax.map(slab_attention, (queries, key_head_rows, value_head_rows, counts))
    mixed_out = low(low_back(mixed_out.reshape(TOKB, QUERY_HEADS * HEAD_SIZE)))
    hidden_state = block_in + low_back(jnp.dot(mixed_out, w_out, precision=highest_precision))
    normed_ffn = low(rms_norm(hidden_state, gain_ffn))
    gate_pre = low_back(jnp.dot(normed_ffn, w_gate, precision=highest_precision))
    up_pre = low_back(jnp.dot(normed_ffn, w_up, precision=highest_precision))
    hidden = low(jax.nn.silu(gate_pre) * up_pre)
    return hidden_state + low_back(jnp.dot(hidden, w_down, precision=highest_precision))

def reference(inputs, lengths, gain_attn, w_query, key_weight, value_weight, w_out, gain_ffn, w_gate, w_up, w_down, cotangent):
    params = tuple((weight.astype(jnp.float32) for weight in (gain_attn, w_query, key_weight, value_weight, w_out, gain_ffn, w_gate, w_up, w_down)))

    def forward(inputs_f, *weights):

        def one_batch(pieces):
            return decoder_layer(pieces, weights)
        return lax.map(jax.checkpoint(one_batch), (inputs_f, lengths))
    outputs, pullback = jax.vjp(forward, inputs.astype(jnp.float32), *params)
    grads = pullback(cotangent.astype(jnp.float32))
    return (outputs.astype(jnp.bfloat16), grads[0], grads[1], grads[2], grads[3], grads[4], grads[5], grads[6], grads[7], grads[8], grads[9])
```

```python
import jax
import jax.numpy as jnp
from jax import lax
from jax.sharding import PartitionSpec as P

QUERY_HEADS = 32
KEY_VALUE_HEADS = 4
HEAD_SIZE = 64
QUERY_ROWS = 512

eps_norm = 1e-05
rope_base = 10000.0
F32 = jnp.float32
BF16 = jnp.bfloat16


def slab_layout(counts, extent):
    bounds = jnp.cumsum(counts)
    places = jnp.arange(extent, dtype=jnp.int32)
    passed = (places[:, None] >= bounds[None, :]).astype(jnp.int32)
    segment = jnp.sum(passed, axis=1)
    offsets = jnp.sum(passed * counts[None, :], axis=1)
    return (segment, places - offsets)


def rope_tables(positions, head_dim):
    half_dim = head_dim // 2
    frequency = jnp.exp(
        -jnp.log(rope_base) * (2.0 * jnp.arange(half_dim, dtype=F32) / head_dim)
    )
    angles = positions.astype(F32)[:, None] * frequency[None, :]
    return (jnp.cos(angles)[:, None, :], jnp.sin(angles)[:, None, :])


def rotate(tensor, cosine_table, sine_table):
    half_dim = tensor.shape[-1] // 2
    first_half = tensor[..., :half_dim]
    second_half = tensor[..., half_dim:]
    return jnp.concatenate(
        [
            first_half * cosine_table - second_half * sine_table,
            second_half * cosine_table + first_half * sine_table,
        ],
        axis=-1,
    )


def dot_nn(left_side, right_side, out=F32):
    return lax.dot_general(
        left_side, right_side, (((1,), (0,)), ((), ())), preferred_element_type=F32
    ).astype(out)


def dot_nt(left_side, right_side, out=F32):
    return lax.dot_general(
        left_side, right_side, (((1,), (1,)), ((), ())), preferred_element_type=F32
    ).astype(out)


def dot_tn(left_side, right_side):
    return lax.dot_general(
        left_side, right_side, (((0,), (0,)), ((), ())), preferred_element_type=F32
    )


def gather_rows(part):
    return lax.all_gather(part, "rows", axis=0, tiled=True)


def scatter_rows(partial_sum):
    return lax.psum_scatter(partial_sum, "rows", scatter_dimension=0, tiled=True).astype(F32)


def gather_cols(part):
    return lax.all_gather(part, "cols", axis=0, tiled=True)


def scatter_cols(partial_sum):
    return lax.psum_scatter(
        partial_sum.astype(BF16), "cols", scatter_dimension=0, tiled=True
    ).astype(F32)


def to_tokens(array, n_rows, n_cols):
    own_rows, own_features = array.shape
    lead = array.reshape(n_rows, own_rows // n_rows, own_features)
    lead = lax.all_to_all(lead, "rows", 0, 0, tiled=True)
    lead = lead.reshape(n_cols, own_rows // n_cols, own_features)
    lead = lax.all_to_all(lead, "cols", 0, 0, tiled=True)
    return jnp.transpose(lead, (1, 0, 2)).reshape(own_rows // n_cols, n_cols * own_features)


def from_tokens(array, n_rows, n_cols):
    few_rows, features = array.shape
    lead = jnp.transpose(array.reshape(few_rows, n_cols, features // n_cols), (1, 0, 2))
    lead = lax.all_to_all(lead, "cols", 0, 0, tiled=True)
    lead = lead.reshape(n_rows, few_rows * n_cols // n_rows, features // n_cols)
    lead = lax.all_to_all(lead, "rows", 0, 0, tiled=True)
    return lead.reshape(few_rows * n_cols, features // n_cols)


def key_mask(segment, first, block_rows):
    last = first + block_rows
    query_places = first + jnp.arange(block_rows, dtype=jnp.int32)
    places = jnp.arange(last, dtype=jnp.int32)
    same = segment[first:last, None] == segment[None, :last]
    return same & (places[None, :] <= query_places[:, None])


def attention_forward(queries, key_rot, value_rows, segment):
    extent = queries.shape[1]
    block_rows = min(QUERY_ROWS, extent)
    scaling = queries.shape[-1] ** (-0.5)
    outs, totals = [], []
    for first in range(0, extent, block_rows):
        last = first + block_rows
        scores = (
            jnp.einsum(
                "hqd,kd->hqk",
                queries[:, first:last],
                key_rot[:last],
                preferred_element_type=F32,
            )
            * scaling
        )
        scores = jnp.where(key_mask(segment, first, block_rows)[None], scores, -1e30)
        row_peak = jnp.max(scores, axis=2, keepdims=True)
        shifted = jnp.exp(scores - row_peak)
        row_total = jnp.sum(shifted, axis=2, keepdims=True)
        probs = (shifted / row_total).astype(BF16)
        outs.append(
            jnp.einsum("hqk,kd->qhd", probs, value_rows[:last], preferred_element_type=F32)
        )
        totals.append(row_peak + jnp.log(row_total))
    return (jnp.concatenate(outs, axis=0).astype(BF16), totals)


def attention_backward(queries, key_rot, value_rows, segment, totals, grad_mixed):
    heads, extent, head_dim = queries.shape
    block_rows = min(QUERY_ROWS, extent)
    scaling = head_dim ** (-0.5)
    grad_queries = []
    grad_keys = jnp.zeros((extent, head_dim), F32)
    grad_values = jnp.zeros((extent, head_dim), F32)
    for first, total in zip(range(0, extent, block_rows), totals):
        last = first + block_rows
        query_block = queries[:, first:last]
        grad_block = grad_mixed[:, first:last]
        keys, values = key_rot[:last], value_rows[:last]
        scores = (
            jnp.einsum("hqd,kd->hqk", query_block, keys, preferred_element_type=F32) * scaling
        )
        scores = jnp.where(key_mask(segment, first, block_rows)[None], scores, -1e30)
        probs = jnp.exp(scores - total)
        grad_probs = jnp.einsum("hqd,kd->hqk", grad_block, values, preferred_element_type=F32)
        inner_sum = jnp.sum(grad_probs * probs, axis=2, keepdims=True)
        grad_scores = (probs * (grad_probs - inner_sum)).astype(BF16)
        grad_queries.append(
            jnp.einsum("hqk,kd->qhd", grad_scores, keys, preferred_element_type=F32) * scaling
        )
        rest = ((0, extent - last), (0, 0))
        grad_keys = grad_keys + jnp.pad(
            jnp.einsum("hqk,hqd->kd", grad_scores, query_block, preferred_element_type=F32)
            * scaling,
            rest,
        )
        grad_values = grad_values + jnp.pad(
            jnp.einsum(
                "hqk,hqd->kd", probs.astype(BF16), grad_block, preferred_element_type=F32
            ),
            rest,
        )
    return (jnp.concatenate(grad_queries, axis=0), grad_keys, grad_values)


def norm_backward(grad_in, normed, inverse_rms, gain):
    scaled = grad_in * gain[None, :]
    row_mean = jnp.mean(scaled * normed, axis=1, keepdims=True)
    return (
        inverse_rms * (scaled - normed * row_mean),
        jnp.sum(grad_in * normed, axis=0),
    )


def local(
    inputs,
    lengths,
    gain_attn,
    w_query,
    key_weight,
    value_weight,
    w_out,
    gain_ffn,
    w_gate,
    w_up,
    w_down,
    cotangent,
):
    n_rows, n_cols = lax.axis_size("rows"), lax.axis_size("cols")
    batches, own_rows, _ = inputs.shape
    sub_rows = own_rows // n_rows
    per_block = n_rows // n_cols
    slab_rows = own_rows * n_rows // n_cols
    head_dim = HEAD_SIZE
    query_width = w_query.shape[1]
    ffn_width = w_gate.shape[1]
    heads = query_width // head_dim
    proj_width = query_width + 2 * head_dim
    local_head = lax.axis_index("rows") * heads // (QUERY_HEADS // KEY_VALUE_HEADS)
    key_own = lax.dynamic_slice_in_dim(key_weight, local_head * head_dim, head_dim, 1)
    value_own = lax.dynamic_slice_in_dim(value_weight, local_head * head_dim, head_dim, 1)

    def ordered(array):
        wide = array.reshape(n_rows, per_block, sub_rows, -1)
        return jnp.transpose(wide, (1, 0, 2, 3)).reshape(slab_rows, -1)

    def reordered(array):
        wide = array.reshape(per_block, n_rows, sub_rows, -1)
        return jnp.transpose(wide, (1, 0, 2, 3)).reshape(slab_rows, -1)

    def by_head(array):
        return jnp.transpose(array.reshape(slab_rows, heads, head_dim), (1, 0, 2))

    rows_in = [to_tokens(inputs[m], n_rows, n_cols) for m in range(batches)]
    packed = gather_cols(
        jnp.concatenate(
            [w_query, key_own, value_own, gain_attn[:, None], gain_ffn[:, None]], axis=1
        )
    )
    proj_w = packed[:, :proj_width]
    gain_one = packed[:, proj_width].astype(F32)
    gain_two = packed[:, proj_width + 1].astype(F32)
    out_w = gather_cols(w_out.T)
    gate_up_w = gather_cols(jnp.concatenate([w_gate, w_up], axis=1))
    down_w = gather_cols(w_down.T)
    rows_dy = [to_tokens(cotangent[m], n_rows, n_cols) for m in range(batches)]

    kept = []
    results = []
    for m in range(batches):
        row_in = rows_in[m].astype(F32)
        inverse_one = lax.rsqrt(jnp.mean(row_in * row_in, axis=1, keepdims=True) + eps_norm)
        normed_one = row_in * inverse_one
        all_one = gather_rows((normed_one * gain_one[None, :]).astype(BF16))
        segment, positions = slab_layout(lengths[m, 0], slab_rows)
        cosine_table, sine_table = rope_tables(positions, head_dim)
        projected = ordered(dot_nn(all_one, proj_w))
        queries = rotate(
            projected[:, :query_width].reshape(slab_rows, heads, head_dim),
            cosine_table,
            sine_table,
        ).astype(BF16)
        queries = jnp.transpose(queries, (1, 0, 2))
        key_rot = rotate(
            projected[:, None, query_width : query_width + head_dim], cosine_table, sine_table
        )[:, 0].astype(BF16)
        value_rows = projected[:, query_width + head_dim :].astype(BF16)
        mixed, totals = attention_forward(queries, key_rot, value_rows, segment)
        mixed = reordered(mixed.reshape(slab_rows, query_width))
        hidden_state = row_in + scatter_rows(dot_nt(mixed, out_w, BF16))
        inverse_two = lax.rsqrt(
            jnp.mean(hidden_state * hidden_state, axis=1, keepdims=True) + eps_norm
        )
        normed_two = hidden_state * inverse_two
        all_two = gather_rows((normed_two * gain_two[None, :]).astype(BF16))
        gate_both = dot_nn(all_two, gate_up_w)
        gate_pre, upward = gate_both[:, :ffn_width], gate_both[:, ffn_width:]
        gate_sigma = jax.nn.sigmoid(gate_pre)
        hidden = (gate_pre * gate_sigma * upward).astype(BF16)
        result = hidden_state + scatter_rows(dot_nt(hidden, down_w, BF16))
        results.append(from_tokens(result.astype(BF16), n_rows, n_cols))
        kept.append(
            (
                all_one, normed_one, inverse_one, segment, cosine_table, sine_table,
                queries, key_rot, value_rows, mixed, totals, normed_two, inverse_two,
                all_two, gate_both, hidden,
            )
        )

    sums = None
    grad_inputs = []
    for m in range(batches):
        (
            all_one, normed_one, inverse_one, segment, cosine_table, sine_table,
            queries, key_rot, value_rows, mixed, totals, normed_two, inverse_two,
            all_two, gate_both, hidden,
        ) = kept[m]
        all_dy = gather_rows(rows_dy[m])
        grad_down = dot_tn(all_dy, hidden)
        grad_hidden = dot_nn(all_dy, down_w)
        gate_pre, upward = gate_both[:, :ffn_width], gate_both[:, ffn_width:]
        gate_sigma = jax.nn.sigmoid(gate_pre)
        grad_gate = grad_hidden * upward * gate_sigma * (1.0 + gate_pre * (1.0 - gate_sigma))
        grad_up = grad_hidden * gate_pre * gate_sigma
        grad_both = jnp.concatenate([grad_gate.astype(BF16), grad_up.astype(BF16)], axis=1)
        grad_gu = dot_tn(all_two, grad_both)
        grad_two, gain_two_part = norm_backward(
            scatter_rows(dot_nt(grad_both, gate_up_w, BF16)), normed_two, inverse_two, gain_two
        )
        grad_state = grad_two + rows_dy[m].astype(F32)
        all_dh = gather_rows(grad_state.astype(BF16))
        grad_out = dot_tn(all_dh, mixed)
        grad_mixed = by_head(ordered(dot_nn(all_dh, out_w, BF16)))
        grad_q, grad_k, grad_v = attention_backward(
            queries, key_rot, value_rows, segment, totals, grad_mixed
        )
        back_q = rotate(grad_q, cosine_table, -sine_table).reshape(slab_rows, query_width)
        back_k = rotate(grad_k[:, None, :], cosine_table, -sine_table)[:, 0, :]
        grad_qkv = reordered(jnp.concatenate([back_q, back_k, grad_v], axis=1).astype(BF16))
        grad_proj = dot_tn(all_one, grad_qkv)
        grad_one, gain_one_part = norm_backward(
            scatter_rows(dot_nt(grad_qkv, proj_w, BF16)), normed_one, inverse_one, gain_one
        )
        grad_inputs.append(
            from_tokens((grad_one + grad_state).astype(BF16), n_rows, n_cols).astype(F32)
        )
        terms = (
            grad_down,
            grad_gu,
            grad_out,
            jnp.concatenate(
                [grad_proj, gain_one_part[:, None], gain_two_part[:, None]], axis=1
            ),
        )
        sums = terms if sums is None else tuple(a + b for a, b in zip(sums, terms))

    grad_down = scatter_cols(sums[0])
    grad_gu = scatter_cols(sums[1])
    grad_out = scatter_cols(sums[2])
    grad_proj = scatter_cols(sums[3])
    shared = gather_rows(grad_proj[None, :, query_width:].astype(BF16)).astype(F32)
    copies = shared.reshape(KEY_VALUE_HEADS, n_rows // KEY_VALUE_HEADS, *shared.shape[1:])
    heads_sum = jnp.sum(copies, axis=1)
    key_sum = jnp.transpose(heads_sum[:, :, :head_dim], (1, 0, 2)).reshape(key_weight.shape)
    value_sum = jnp.transpose(heads_sum[:, :, head_dim : 2 * head_dim], (1, 0, 2)).reshape(
        value_weight.shape
    )
    gains = jnp.sum(heads_sum[:, :, 2 * head_dim :], axis=0)
    return (
        jnp.stack(results),
        jnp.stack(grad_inputs),
        gains[:, 0],
        grad_proj[:, :query_width],
        key_sum,
        value_sum,
        grad_out.T,
        gains[:, 1],
        grad_gu[:, :ffn_width],
        grad_gu[:, ffn_width:],
        grad_down.T,
    )


def solution(mesh):
    in_specs = (
        P(None, "rows", "cols"),
        P(None, "cols", None),
        P("cols"),
        P("cols", "rows"),
        P("cols", None),
        P("cols", None),
        P("rows", "cols"),
        P("cols"),
        P("cols", "rows"),
        P("cols", "rows"),
        P("rows", "cols"),
        P(None, "rows", "cols"),
    )
    out_specs = (
        P(None, "rows", "cols"),
        P(None, "rows", "cols"),
        P("cols"),
        P("cols", "rows"),
        P("cols", None),
        P("cols", None),
        P("rows", "cols"),
        P("cols"),
        P("cols", "rows"),
        P("cols", "rows"),
        P("rows", "cols"),
    )
    return jax.shard_map(local, mesh=mesh, in_specs=in_specs, out_specs=out_specs, check_vma=False)
```

```python
import jax
import jax.numpy as jnp
from jax import lax
from jax.sharding import PartitionSpec as P

QUERY_HEADS = 32
KEY_VALUE_HEADS = 4
HEAD_SIZE = 64
QUERY_ROWS = 512

eps_norm = 1e-05
rope_base = 10000.0
F32 = jnp.float32
BF16 = jnp.bfloat16


def slab_layout(counts, extent):
    bounds = jnp.cumsum(counts)
    places = jnp.arange(extent, dtype=jnp.int32)
    passed = (places[:, None] >= bounds[None, :]).astype(jnp.int32)
    segment = jnp.sum(passed, axis=1)
    offsets = jnp.sum(passed * counts[None, :], axis=1)
    return (segment, places - offsets)


def rope_tables(positions, head_dim):
    half_dim = head_dim // 2
    frequency = jnp.exp(
        -jnp.log(rope_base) * (2.0 * jnp.arange(half_dim, dtype=F32) / head_dim)
    )
    angles = positions.astype(F32)[:, None] * frequency[None, :]
    return (jnp.cos(angles)[:, None, :], jnp.sin(angles)[:, None, :])


def rotate(tensor, cosine_table, sine_table):
    half_dim = tensor.shape[-1] // 2
    first_half = tensor[..., :half_dim]
    second_half = tensor[..., half_dim:]
    return jnp.concatenate(
        [
            first_half * cosine_table - second_half * sine_table,
            second_half * cosine_table + first_half * sine_table,
        ],
        axis=-1,
    )


def dot_nn(left_side, right_side, out=F32):
    return lax.dot_general(
        left_side, right_side, (((1,), (0,)), ((), ())), preferred_element_type=F32
    ).astype(out)


def dot_nt(left_side, right_side, out=F32):
    return lax.dot_general(
        left_side, right_side, (((1,), (1,)), ((), ())), preferred_element_type=F32
    ).astype(out)


def dot_tn(left_side, right_side):
    return lax.dot_general(
        left_side, right_side, (((0,), (0,)), ((), ())), preferred_element_type=F32
    )


def swapped(part, bit):
    count = lax.axis_size("rows")
    return lax.ppermute(part, "rows", [(i, i ^ bit) for i in range(count)])


def gather_rows(part):
    count = lax.axis_size("rows")
    half = part.shape[0] // 2
    whole = {0: (part[:half], part[half:])}
    blocks = [[part]]
    for place in range(2, count, 2):
        high = 1 << (place.bit_length() - 1)
        low = place & -place
        if high == low:
            block = swapped(part, high)
            blocks.append([block])
            whole[place] = (block[:half], block[half:])
        else:
            whole[place] = (
                swapped(whole[place ^ high][0], high),
                swapped(whole[place ^ low][1], low),
            )
            blocks.append(list(whole[place]))
    near = [piece for block in blocks for piece in block]
    return jnp.concatenate(near + [swapped(piece, 1) for piece in near], axis=0)


def scatter_rows(left_side, weight):
    chips = lax.axis_size("rows") // 2
    middle = left_side.shape[0] // 2
    n = middle // chips
    half = n // 2
    sent = swapped(dot_nt(left_side[middle:], weight, BF16), 1)
    own = dot_nt(left_side[:middle], weight, BF16)
    chip_bits = [1 << b for b in range(chips.bit_length() - 1)]
    finished = []
    for side, order in enumerate((chip_bits, chip_bits[::-1])):
        held = {}
        for chip in range(chips):
            rows = slice(chip * n + side * half, chip * n + (side + 1) * half)
            held[chip] = own[rows].astype(F32) + sent[rows].astype(F32)
        for bit in order:
            leaving = [chip for chip in held if chip & bit]
            got = swapped(
                jnp.concatenate([held[chip].astype(BF16) for chip in leaving], axis=0), 2 * bit
            )
            for at, chip in enumerate(leaving):
                del held[chip]
                held[chip ^ bit] = held[chip ^ bit] + got[at * half : (at + 1) * half].astype(F32)
        finished.append(held[0])
    return jnp.concatenate(finished, axis=0)


def gather_cols(part):
    return lax.all_gather(part, "cols", axis=0, tiled=True)


def scatter_cols(partial_sum):
    return lax.psum_scatter(
        partial_sum.astype(BF16), "cols", scatter_dimension=0, tiled=True
    ).astype(F32)


def to_tokens(arrays, n_rows, n_cols):
    count = len(arrays)
    own_rows, own_features = arrays[0].shape
    lead = jnp.stack([a.reshape(n_rows, -1, own_features) for a in arrays], axis=1)
    lead = lax.all_to_all(lead, "rows", 0, 0, tiled=True)
    per_block = n_rows // n_cols
    lead = lead.reshape(n_cols, per_block, count, own_rows // n_rows, own_features)
    lead = lax.all_to_all(lead, "cols", 0, 0, tiled=True)
    lead = jnp.transpose(lead, (2, 1, 3, 0, 4))
    return list(lead.reshape(count, own_rows // n_cols, n_cols * own_features))


def from_tokens(arrays, n_rows, n_cols):
    count = len(arrays)
    few_rows, features = arrays[0].shape
    per_block = n_rows // n_cols
    sub_rows = few_rows // per_block
    own_features = features // n_cols
    lead = jnp.stack(
        [a.reshape(per_block, sub_rows, n_cols, own_features) for a in arrays], axis=1
    )
    lead = jnp.transpose(lead, (3, 0, 1, 2, 4))
    lead = lax.all_to_all(lead, "cols", 0, 0, tiled=True)
    lead = lead.reshape(n_rows, count, sub_rows, own_features)
    lead = lax.all_to_all(lead, "rows", 0, 0, tiled=True)
    return list(jnp.swapaxes(lead, 0, 1).reshape(count, n_rows * sub_rows, own_features))


def key_mask(segment, first, block_rows):
    last = first + block_rows
    query_places = first + jnp.arange(block_rows, dtype=jnp.int32)
    places = jnp.arange(last, dtype=jnp.int32)
    same = segment[first:last, None] == segment[None, :last]
    return same & (places[None, :] <= query_places[:, None])


def attention_forward(queries, key_rot, value_rows, segment):
    extent = queries.shape[1]
    block_rows = min(QUERY_ROWS, extent)
    scaling = queries.shape[-1] ** (-0.5)
    outs, totals = [], []
    for first in range(0, extent, block_rows):
        last = first + block_rows
        scores = (
            jnp.einsum(
                "hqd,kd->hqk",
                queries[:, first:last],
                key_rot[:last],
                preferred_element_type=F32,
            )
            * scaling
        )
        scores = jnp.where(key_mask(segment, first, block_rows)[None], scores, -1e30)
        row_peak = jnp.max(scores, axis=2, keepdims=True)
        shifted = jnp.exp(scores - row_peak)
        row_total = jnp.sum(shifted, axis=2, keepdims=True)
        probs = (shifted / row_total).astype(BF16)
        outs.append(
            jnp.einsum("hqk,kd->qhd", probs, value_rows[:last], preferred_element_type=F32)
        )
        totals.append(row_peak + jnp.log(row_total))
    return (jnp.concatenate(outs, axis=0).astype(BF16), totals)


def attention_backward(queries, key_rot, value_rows, segment, totals, grad_mixed):
    heads, extent, head_dim = queries.shape
    block_rows = min(QUERY_ROWS, extent)
    scaling = head_dim ** (-0.5)
    grad_queries = []
    grad_keys = jnp.zeros((extent, head_dim), F32)
    grad_values = jnp.zeros((extent, head_dim), F32)
    for first, total in zip(range(0, extent, block_rows), totals):
        last = first + block_rows
        query_block = queries[:, first:last]
        grad_block = grad_mixed[:, first:last]
        keys, values = key_rot[:last], value_rows[:last]
        scores = (
            jnp.einsum("hqd,kd->hqk", query_block, keys, preferred_element_type=F32) * scaling
        )
        scores = jnp.where(key_mask(segment, first, block_rows)[None], scores, -1e30)
        probs = jnp.exp(scores - total)
        grad_probs = jnp.einsum("hqd,kd->hqk", grad_block, values, preferred_element_type=F32)
        inner_sum = jnp.sum(grad_probs * probs, axis=2, keepdims=True)
        grad_scores = (probs * (grad_probs - inner_sum)).astype(BF16)
        grad_queries.append(
            jnp.einsum("hqk,kd->qhd", grad_scores, keys, preferred_element_type=F32) * scaling
        )
        rest = ((0, extent - last), (0, 0))
        grad_keys = grad_keys + jnp.pad(
            jnp.einsum("hqk,hqd->kd", grad_scores, query_block, preferred_element_type=F32)
            * scaling,
            rest,
        )
        grad_values = grad_values + jnp.pad(
            jnp.einsum(
                "hqk,hqd->kd", probs.astype(BF16), grad_block, preferred_element_type=F32
            ),
            rest,
        )
    return (jnp.concatenate(grad_queries, axis=0), grad_keys, grad_values)


def after(value, other):
    return lax.optimization_barrier((value, other))[0]


def norm_backward(grad_in, normed, inverse_rms, gain):
    scaled = grad_in * gain[None, :]
    row_mean = jnp.mean(scaled * normed, axis=1, keepdims=True)
    return (
        inverse_rms * (scaled - normed * row_mean),
        jnp.sum(grad_in * normed, axis=0),
    )


def local(
    inputs,
    lengths,
    gain_attn,
    w_query,
    key_weight,
    value_weight,
    w_out,
    gain_ffn,
    w_gate,
    w_up,
    w_down,
    cotangent,
):
    n_rows, n_cols = lax.axis_size("rows"), lax.axis_size("cols")
    batches, own_rows, _ = inputs.shape
    sub_rows = own_rows // n_rows
    per_block = n_rows // n_cols
    slab_rows = own_rows * n_rows // n_cols
    head_dim = HEAD_SIZE
    query_width = w_query.shape[1]
    ffn_width = w_gate.shape[1]
    heads = query_width // head_dim
    proj_width = query_width + 2 * head_dim
    local_head = lax.axis_index("rows") * heads // (QUERY_HEADS // KEY_VALUE_HEADS)
    key_own = lax.dynamic_slice_in_dim(key_weight, local_head * head_dim, head_dim, 1)
    value_own = lax.dynamic_slice_in_dim(value_weight, local_head * head_dim, head_dim, 1)

    own_row = lax.axis_index("rows")

    def ordered(array):
        wide = array.reshape(n_rows, per_block, sub_rows, -1)
        pieces = []
        for row in range(n_rows):
            place = own_row ^ row
            place = (place & 1) * (n_rows // 2) + place // 2
            pieces.append(lax.dynamic_slice_in_dim(wide, place, 1, 0)[0])
        return jnp.stack(pieces, axis=1).reshape(slab_rows, -1)

    def reordered(array):
        wide = array.reshape(per_block, n_rows, sub_rows, -1)
        pieces = []
        for place in range(n_rows):
            apart = (place % (n_rows // 2)) * 2 + place // (n_rows // 2)
            pieces.append(lax.dynamic_slice_in_dim(wide, own_row ^ apart, 1, 1)[:, 0])
        return jnp.stack(pieces, axis=0).reshape(slab_rows, -1)

    def by_head(array):
        return jnp.transpose(array.reshape(slab_rows, heads, head_dim), (1, 0, 2))

    rows_in = to_tokens([inputs[0]], n_rows, n_cols)
    packed = gather_cols(
        jnp.concatenate(
            [w_query, key_own, value_own, gain_attn[:, None], gain_ffn[:, None]], axis=1
        )
    )
    proj_w = packed[:, :proj_width]
    gain_one = packed[:, proj_width].astype(F32)
    gain_two = packed[:, proj_width + 1].astype(F32)
    out_w = gather_cols(w_out.T)
    gate_up_w = gather_cols(jnp.concatenate([w_gate, w_up], axis=1))
    down_w = gather_cols(w_down.T)
    rest = [inputs[m] for m in range(1, batches)] + [cotangent[m] for m in range(batches)]
    rest = to_tokens(rest, n_rows, n_cols)
    rows_in += rest[: batches - 1]
    rows_dy = rest[batches - 1 :]

    kept = []
    results = []
    for m in range(batches):
        entered = rows_in[m] if m == 0 else after(rows_in[m], kept[-1][15])
        row_in = entered.astype(F32)
        inverse_one = lax.rsqrt(jnp.mean(row_in * row_in, axis=1, keepdims=True) + eps_norm)
        normed_one = row_in * inverse_one
        all_one = gather_rows((normed_one * gain_one[None, :]).astype(BF16))
        segment, positions = slab_layout(lengths[m, 0], slab_rows)
        cosine_table, sine_table = rope_tables(positions, head_dim)
        projected = ordered(dot_nn(all_one, proj_w))
        queries = rotate(
            projected[:, :query_width].reshape(slab_rows, heads, head_dim),
            cosine_table,
            sine_table,
        ).astype(BF16)
        queries = jnp.transpose(queries, (1, 0, 2))
        key_rot = rotate(
            projected[:, None, query_width : query_width + head_dim], cosine_table, sine_table
        )[:, 0].astype(BF16)
        value_rows = projected[:, query_width + head_dim :].astype(BF16)
        mixed, totals = attention_forward(queries, key_rot, value_rows, segment)
        mixed = reordered(mixed.reshape(slab_rows, query_width))
        hidden_state = row_in + scatter_rows(mixed, out_w)
        inverse_two = lax.rsqrt(
            jnp.mean(hidden_state * hidden_state, axis=1, keepdims=True) + eps_norm
        )
        normed_two = hidden_state * inverse_two
        all_two = gather_rows((normed_two * gain_two[None, :]).astype(BF16))
        gate_both = dot_nn(all_two, gate_up_w)
        gate_pre, upward = gate_both[:, :ffn_width], gate_both[:, ffn_width:]
        gate_sigma = jax.nn.sigmoid(gate_pre)
        hidden = (gate_pre * gate_sigma * upward).astype(BF16)
        result = hidden_state + scatter_rows(hidden, down_w)
        results.append(result.astype(BF16))
        kept.append(
            (
                all_one, normed_one, inverse_one, segment, cosine_table, sine_table,
                queries, key_rot, value_rows, mixed, totals, normed_two, inverse_two,
                all_two, gate_both.astype(BF16), hidden,
            )
        )

    sums = {}
    grad_inputs = []
    for m in range(batches):
        (
            all_one, normed_one, inverse_one, segment, cosine_table, sine_table,
            queries, key_rot, value_rows, mixed, totals, normed_two, inverse_two,
            all_two, gate_both, hidden,
        ) = kept[m]
        start = hidden if m == 0 else (hidden, grad_state)
        all_dy = gather_rows(after(rows_dy[m], start))
        grad_down = dot_tn(all_dy, hidden)
        grad_hidden = dot_nn(all_dy, down_w)
        gate_pre = gate_both[:, :ffn_width].astype(F32)
        upward = gate_both[:, ffn_width:].astype(F32)
        gate_sigma = jax.nn.sigmoid(gate_pre)
        grad_gate = grad_hidden * upward * gate_sigma * (1.0 + gate_pre * (1.0 - gate_sigma))
        grad_up = grad_hidden * gate_pre * gate_sigma
        grad_both = jnp.concatenate([grad_gate.astype(BF16), grad_up.astype(BF16)], axis=1)
        grad_gu = dot_tn(all_two, grad_both)
        grad_two, gain_two_part = norm_backward(
            scatter_rows(grad_both, gate_up_w), normed_two, inverse_two, gain_two
        )
        grad_state = grad_two + rows_dy[m].astype(F32)
        final = m == batches - 1
        sums["down"] = grad_down if m == 0 else sums["down"] + grad_down
        sums["gu"] = grad_gu if m == 0 else sums["gu"] + grad_gu
        entering = grad_state.astype(BF16)
        if final:
            grad_down = scatter_cols(sums["down"])
            grad_gu = scatter_cols(sums["gu"])
            entering = after(entering, grad_down)
        all_dh = gather_rows(entering)
        grad_out = dot_tn(all_dh, mixed)
        sums["out"] = grad_out if m == 0 else sums["out"] + grad_out
        if final:
            grad_out = scatter_cols(sums["out"])
        grad_mixed = by_head(ordered(dot_nn(all_dh, out_w, BF16)))
        grad_q, grad_k, grad_v = attention_backward(
            queries, key_rot, value_rows, segment, totals, grad_mixed
        )
        back_q = rotate(grad_q, cosine_table, -sine_table).reshape(slab_rows, query_width)
        back_k = rotate(grad_k[:, None, :], cosine_table, -sine_table)[:, 0, :]
        grad_qkv = jnp.concatenate([back_q, back_k, grad_v], axis=1).astype(BF16)
        if final:
            early = from_tokens(results + grad_inputs, n_rows, n_cols)
            grad_qkv = after(grad_qkv, early)
        grad_qkv = reordered(grad_qkv)
        grad_proj = dot_tn(all_one, grad_qkv)
        grad_one, gain_one_part = norm_backward(
            scatter_rows(grad_qkv, proj_w), normed_one, inverse_one, gain_one
        )
        grad_input = (grad_one + grad_state).astype(BF16)
        if final:
            grad_input = after(grad_input, (grad_gu, grad_out))
        grad_inputs.append(grad_input)
        terms = jnp.concatenate(
            [grad_proj, gain_one_part[:, None], gain_two_part[:, None]], axis=1
        )
        sums["proj"] = terms if m == 0 else sums["proj"] + terms

    late = from_tokens(grad_inputs[-1:], n_rows, n_cols)
    results = early[:batches]
    grad_inputs = [a.astype(F32) for a in early[batches:] + late]
    grad_proj = scatter_cols(sums["proj"])
    shared = lax.all_gather(
        grad_proj[:, query_width:].astype(BF16), "rows", axis=0
    ).astype(F32)
    copies = shared.reshape(KEY_VALUE_HEADS, n_rows // KEY_VALUE_HEADS, *shared.shape[1:])
    heads_sum = jnp.sum(copies, axis=1)
    key_sum = jnp.transpose(heads_sum[:, :, :head_dim], (1, 0, 2)).reshape(key_weight.shape)
    value_sum = jnp.transpose(heads_sum[:, :, head_dim : 2 * head_dim], (1, 0, 2)).reshape(
        value_weight.shape
    )
    gains = jnp.sum(heads_sum[:, :, 2 * head_dim :], axis=0)
    return (
        jnp.stack(results),
        jnp.stack(grad_inputs),
        gains[:, 0],
        grad_proj[:, :query_width],
        key_sum,
        value_sum,
        grad_out.T,
        gains[:, 1],
        grad_gu[:, :ffn_width],
        grad_gu[:, ffn_width:],
        grad_down.T,
    )


def solution(mesh):
    in_specs = (
        P(None, "rows", "cols"),
        P(None, "cols", None),
        P("cols"),
        P("cols", "rows"),
        P("cols", None),
        P("cols", None),
        P("rows", "cols"),
        P("cols"),
        P("cols", "rows"),
        P("cols", "rows"),
        P("rows", "cols"),
        P(None, "rows", "cols"),
    )
    out_specs = (
        P(None, "rows", "cols"),
        P(None, "rows", "cols"),
        P("cols"),
        P("cols", "rows"),
        P("cols", None),
        P("cols", None),
        P("rows", "cols"),
        P("cols"),
        P("cols", "rows"),
        P("cols", "rows"),
        P("rows", "cols"),
    )
    return jax.shard_map(local, mesh=mesh, in_specs=in_specs, out_specs=out_specs, check_vma=False)
```

```python
import functools

import jax
import jax.numpy as jnp
from jax import lax
from jax.experimental import pallas as pl
from jax.experimental.pallas import tpu as pltpu
from jax.sharding import PartitionSpec as P

QUERY_HEADS = 32
KEY_VALUE_HEADS = 4
HEAD_SIZE = 64
QUERY_ROWS = 256

eps_norm = 1e-05
rope_base = 10000.0
F32 = jnp.float32
BF16 = jnp.bfloat16


def slab_layout(counts, places):
    bounds = jnp.cumsum(counts)
    passed = (places[:, None] >= bounds[None, :]).astype(jnp.int32)
    return places - jnp.sum(passed * counts[None, :], axis=1)


def rope_tables(positions, head_dim):
    half_dim = head_dim // 2
    frequency = jnp.exp(
        -jnp.log(rope_base) * (2.0 * jnp.arange(half_dim, dtype=F32) / head_dim)
    )
    angles = positions.astype(F32)[:, None] * frequency[None, :]
    return (jnp.cos(angles)[:, None, :], jnp.sin(angles)[:, None, :])


def rotate(tensor, cosine_table, sine_table):
    half_dim = tensor.shape[-1] // 2
    first_half = tensor[..., :half_dim]
    second_half = tensor[..., half_dim:]
    return jnp.concatenate(
        [
            first_half * cosine_table - second_half * sine_table,
            second_half * cosine_table + first_half * sine_table,
        ],
        axis=-1,
    )


def dot_nn(left_side, right_side, out=F32):
    return lax.dot_general(
        left_side, right_side, (((1,), (0,)), ((), ())), preferred_element_type=F32
    ).astype(out)


def dot_nt(left_side, right_side, out=F32):
    return lax.dot_general(
        left_side, right_side, (((1,), (1,)), ((), ())), preferred_element_type=F32
    ).astype(out)


def dot_tn(left_side, right_side):
    return lax.dot_general(
        left_side, right_side, (((0,), (0,)), ((), ())), preferred_element_type=F32
    )


def swapped(part, bit):
    count = lax.axis_size("rows")
    return lax.ppermute(part, "rows", [(i, i ^ bit) for i in range(count)])


def chip_order(chips):
    return [place ^ (place >> 1) for place in range(chips)]


def gather_rows(part):
    chips = lax.axis_size("rows") // 2
    half = part.shape[0] // 2
    whole = {0: (part[:half], part[half:])}
    blocks = {0: [part]}
    for chip in range(1, chips):
        high = 1 << (chip.bit_length() - 1)
        low = chip & -chip
        if high == low:
            block = swapped(part, 2 * high)
            blocks[chip] = [block]
            whole[chip] = (block[:half], block[half:])
        else:
            whole[chip] = (
                swapped(whole[chip ^ high][0], 2 * high),
                swapped(whole[chip ^ low][1], 2 * low),
            )
            blocks[chip] = list(whole[chip])
    near = jnp.concatenate([x for chip in chip_order(chips) for x in blocks[chip]], axis=0)
    return (near, swapped(near, 1))


def scatter_rows(sides, weight):
    chips = lax.axis_size("rows") // 2
    half = sides[0].shape[0] // chips // 2
    sent = swapped(dot_nt(sides[1], weight, BF16), 1).reshape(chips, 2, half, -1)
    own = dot_nt(sides[0], weight, BF16).reshape(chips, 2, half, -1)
    chip_bits = [1 << b for b in range(chips.bit_length() - 1)]
    finished = []
    for side, bits in enumerate((chip_bits, chip_bits[::-1])):
        alive = chip_order(chips)
        places = {chip: at for at, chip in enumerate(alive)}
        got = {chip: [] for chip in alive}

        def total(first, last, extra):
            value = own[first:last, side].astype(F32) + sent[first:last, side].astype(F32)
            for term in extra:
                value = value + term.astype(F32)
            return value

        for step, bit in enumerate(bits):
            leaving = [chip for chip in alive if chip & bit]
            alive = [chip for chip in alive if not chip & bit]
            first, last = places[leaving[0]], places[leaving[-1]] + 1
            if step == 0 and last - first == len(leaving):
                payload = total(first, last, []).astype(BF16)
            else:
                payload = jnp.concatenate(
                    [
                        total(places[chip], places[chip] + 1, got[chip]).astype(BF16)
                        for chip in leaving
                    ],
                    axis=0,
                )
            payload = swapped(payload, 2 * bit)
            for at, chip in enumerate(leaving):
                got[chip ^ bit].append(payload[at : at + 1])
        finished.append(total(0, 1, got[0])[0])
    return jnp.concatenate(finished, axis=0)


def gather_cols(part):
    return lax.all_gather(part, "cols", axis=0, tiled=True)


def scatter_cols(partial_sum):
    return lax.psum_scatter(
        partial_sum.astype(BF16), "cols", scatter_dimension=0, tiled=True
    ).astype(F32)


def gated(value, *signals):
    for signal in signals:
        first = signal[(0,) * signal.ndim].astype(F32)
        value = jnp.where(first > jnp.inf, jnp.zeros_like(value), value)
    return value


def exchange_cols(lead):
    count, own = lax.axis_size("cols"), lax.axis_index("cols")
    pieces = [lax.dynamic_index_in_dim(lead, own, 0, False)]
    for apart in range(1, count):
        piece = lax.dynamic_index_in_dim(lead, own ^ apart, 0, False)
        pieces.append(lax.ppermute(piece, "cols", [(i, i ^ apart) for i in range(count)]))
    bit = 1
    while bit < count:
        swap = (own & bit) != 0
        pieces = [jnp.where(swap, pieces[i ^ bit], pieces[i]) for i in range(count)]
        bit *= 2
    return jnp.stack(pieces)


def to_tokens(arrays, n_rows, n_cols, waits=None):
    count = len(arrays)
    own_rows, own_features = arrays[0].shape
    lead = jnp.stack([a.reshape(n_rows, -1, own_features) for a in arrays], axis=1)
    if waits is not None:
        lead = gated(lead, waits[0])
    lead = lax.all_to_all(lead, "rows", 0, 0, tiled=True)
    per_block = n_rows // n_cols
    lead = lead.reshape(n_cols, per_block, count, own_rows // n_rows, own_features)
    if waits is not None:
        lead = exchange_cols(gated(lead, waits[1]))
    else:
        lead = lax.all_to_all(lead, "cols", 0, 0, tiled=True)
    lead = jnp.transpose(lead, (2, 1, 3, 0, 4))
    return list(lead.reshape(count, own_rows // n_cols, n_cols * own_features))


def from_tokens(arrays, n_rows, n_cols):
    count = len(arrays)
    few_rows, features = arrays[0].shape
    per_block = n_rows // n_cols
    sub_rows = few_rows // per_block
    own_features = features // n_cols
    lead = jnp.stack(
        [a.reshape(per_block, sub_rows, n_cols, own_features) for a in arrays], axis=1
    )
    lead = exchange_cols(jnp.transpose(lead, (3, 0, 1, 2, 4)))
    lead = lead.reshape(n_rows, count, sub_rows, own_features)
    lead = lax.all_to_all(lead, "rows", 0, 0, tiled=True)
    return list(jnp.swapaxes(lead, 0, 1).reshape(count, n_rows * sub_rows, own_features))


def take_in(rows_ref, source, scratch, width, scale):
    blocks, per_block, sub_rows, _ = source.shape
    for place in range(blocks):
        for part in range(per_block):
            first = part * blocks * sub_rows + rows_ref[place] * sub_rows
            first = pl.multiple_of(first, 16)
            value = source[place, part]
            lane = 0
            for target, count, factor in zip(scratch, width, scale):
                for head in range(count):
                    piece = value[:, lane : lane + HEAD_SIZE]
                    if factor is not None:
                        piece = piece * jnp.asarray(factor, BF16)
                    target[head, pl.ds(first, sub_rows), :] = piece
                    lane += HEAD_SIZE


def hand_out(rows_ref, scratch, width, target):
    blocks, per_block, sub_rows, _ = target.shape
    for place in range(blocks):
        for part in range(per_block):
            first = part * blocks * sub_rows + rows_ref[place] * sub_rows
            first = pl.multiple_of(first, 16)
            pieces = [
                source[head, pl.ds(first, sub_rows), :]
                for source, count in zip(scratch, width)
                for head in range(count)
            ]
            target[place, part] = jnp.concatenate(pieces, axis=1)


def masked_scores(query_block, keys, start, first):
    scores = lax.dot_general(
        query_block, keys, (((1,), (1,)), ((), ())), preferred_element_type=F32
    )
    column = lax.broadcasted_iota(jnp.int32, scores.shape, 1)
    row = lax.broadcasted_iota(jnp.int32, scores.shape, 0) + first
    return jnp.where((column <= row) & (column >= start), scores, -1e30)


def forward_kernel(heads, block, rows_ref, start_ref, qkv_ref, out_ref, lse_ref, q_s, k_s, v_s, o_s):
    take_in(
        rows_ref, qkv_ref, (q_s, k_s, v_s), (heads, 1, 1), (HEAD_SIZE ** (-0.5), None, None)
    )
    extent = k_s.shape[1]
    for first in range(0, extent, block):
        last = first + block

        def one_head(head, carry, first=first, last=last):
            scores = masked_scores(
                q_s[head, first:last, :], k_s[0, :last, :], start_ref[first:last, :], first
            )
            row_peak = jnp.max(scores, axis=1, keepdims=True)
            shifted = jnp.exp(scores - row_peak)
            row_total = jnp.sum(shifted, axis=1, keepdims=True)
            probs = (shifted * (1.0 / row_total)).astype(BF16)
            mixed = lax.dot_general(
                probs, v_s[0, :last, :], (((1,), (0,)), ((), ())), preferred_element_type=F32
            )
            o_s[head, first:last, :] = mixed.astype(BF16)
            lse_ref[head, first:last, :] = row_peak + jnp.log(row_total)
            return carry

        lax.fori_loop(0, heads, one_head, 0)
    hand_out(rows_ref, (o_s,), (heads,), out_ref)


def backward_kernel(
    heads, block, rows_ref, start_ref, qkv_ref, lse_ref, grad_ref, out_ref,
    q_s, k_s, v_s, g_s, dq_s, dk_s, dv_s,
):
    scaling = HEAD_SIZE ** (-0.5)
    take_in(rows_ref, qkv_ref, (q_s, k_s, v_s), (heads, 1, 1), (scaling, None, None))
    take_in(rows_ref, grad_ref, (g_s,), (heads,), (None,))
    extent = k_s.shape[1]
    dk_s[...] = jnp.zeros_like(dk_s)
    dv_s[...] = jnp.zeros_like(dv_s)
    for first in range(0, extent, block):
        last = first + block

        def one_head(head, carry, first=first, last=last):
            query_block = q_s[head, first:last, :]
            grad_block = g_s[head, first:last, :]
            keys = k_s[0, :last, :]
            scores = masked_scores(query_block, keys, start_ref[first:last, :], first)
            probs = jnp.exp(scores - lse_ref[head, first:last, :])
            grad_probs = lax.dot_general(
                grad_block, v_s[0, :last, :], (((1,), (1,)), ((), ())),
                preferred_element_type=F32,
            )
            inner_sum = jnp.sum(grad_probs * probs, axis=1, keepdims=True)
            grad_scores = (probs * (grad_probs - inner_sum)).astype(BF16)
            grad_query = lax.dot_general(
                grad_scores, keys, (((1,), (0,)), ((), ())), preferred_element_type=F32
            )
            dq_s[head, first:last, :] = grad_query * scaling
            dk_s[0, :last, :] += lax.dot_general(
                grad_scores, query_block, (((0,), (0,)), ((), ())), preferred_element_type=F32
            )
            dv_s[0, :last, :] += lax.dot_general(
                probs.astype(BF16), grad_block, (((0,), (0,)), ((), ())),
                preferred_element_type=F32,
            )
            return carry

        lax.fori_loop(0, heads, one_head, 0)
    hand_out(rows_ref, (dq_s, dk_s, dv_s), (heads, 1, 1), out_ref)


def call_kernel(body, name, outs, scratch, rows, *operands):
    vmem = pl.BlockSpec(memory_space=pltpu.VMEM)
    flops = 40 * operands[0].shape[0] ** 2 * HEAD_SIZE
    return pl.pallas_call(
        body,
        name=name,
        out_shape=outs,
        in_specs=[pl.BlockSpec(memory_space=pltpu.SMEM)] + [vmem] * len(operands),
        out_specs=[vmem] * len(outs),
        scratch_shapes=scratch,
        cost_estimate=pl.CostEstimate(
            flops=flops, bytes_accessed=8 << 20, transcendentals=4 << 20
        ),
    )(rows, *operands)


def head_scratch(count, extent, dtype):
    return pltpu.VMEM((count, extent, HEAD_SIZE), dtype)


def attention_forward(rows, start, qkv, heads):
    extent = start.shape[0]
    block = min(QUERY_ROWS, extent)
    outs = [
        jax.ShapeDtypeStruct(qkv.shape[:3] + (heads * HEAD_SIZE,), BF16),
        jax.ShapeDtypeStruct((heads, extent, 1), F32),
    ]
    scratch = [head_scratch(count, extent, BF16) for count in (heads, 1, 1, heads)]
    return call_kernel(
        functools.partial(forward_kernel, heads, block),
        "attention_forward", outs, scratch, rows, start, qkv,
    )


def attention_backward(rows, start, qkv, totals, grad_mixed, heads):
    extent = start.shape[0]
    block = min(QUERY_ROWS, extent)
    outs = [jax.ShapeDtypeStruct(qkv.shape, F32)]
    scratch = [head_scratch(count, extent, BF16) for count in (heads, 1, 1, heads)]
    scratch += [head_scratch(count, extent, F32) for count in (heads, 1, 1)]
    return call_kernel(
        functools.partial(backward_kernel, heads, block),
        "attention_backward", outs, scratch, rows, start, qkv, totals, grad_mixed,
    )[0]


def after(value, other):
    return lax.optimization_barrier((value, other))[0]


def norm_backward(grad_in, normed, inverse_rms, gain):
    scaled = grad_in * gain[None, :]
    row_mean = jnp.mean(scaled * normed, axis=1, keepdims=True)
    return (
        inverse_rms * (scaled - normed * row_mean),
        jnp.sum(grad_in * normed, axis=0),
    )


def local(
    inputs,
    lengths,
    gain_attn,
    w_query,
    key_weight,
    value_weight,
    w_out,
    gain_ffn,
    w_gate,
    w_up,
    w_down,
    cotangent,
):
    n_rows, n_cols = lax.axis_size("rows"), lax.axis_size("cols")
    batches, own_rows, _ = inputs.shape
    sub_rows = own_rows // n_rows
    per_block = n_rows // n_cols
    slab_rows = own_rows * n_rows // n_cols
    head_dim = HEAD_SIZE
    query_width = w_query.shape[1]
    ffn_width = w_gate.shape[1]
    heads = query_width // head_dim
    proj_width = query_width + 2 * head_dim
    local_head = lax.axis_index("rows") * heads // (QUERY_HEADS // KEY_VALUE_HEADS)
    key_own = lax.dynamic_slice_in_dim(key_weight, local_head * head_dim, head_dim, 1)
    value_own = lax.dynamic_slice_in_dim(value_weight, local_head * head_dim, head_dim, 1)

    own_row = lax.axis_index("rows")
    chips = n_rows // 2
    order = chip_order(chips)
    apart = jnp.array(
        [2 * order[place % chips] + place // chips for place in range(n_rows)], jnp.int32
    )
    rows = own_row ^ apart
    places = (
        rows[:, None, None] * sub_rows
        + jnp.arange(per_block, dtype=jnp.int32)[None, :, None] * own_rows
        + jnp.arange(sub_rows, dtype=jnp.int32)[None, None, :]
    ).reshape(-1)
    in_order = jnp.arange(slab_rows, dtype=jnp.int32)
    middle = slab_rows // 2
    wide = (n_rows, per_block, sub_rows, -1)

    def halves(array):
        flat = array.reshape(slab_rows, -1)
        return (flat[:middle], flat[middle:])

    def each(function, *sides):
        return tuple(function(*pair) for pair in zip(*sides))

    def outer(left_sides, right_sides):
        return dot_tn(left_sides[0], right_sides[0]) + dot_tn(left_sides[1], right_sides[1])

    def turn(array, cosine_table, sine_table, count):
        heads_part = array[:, : count * head_dim].reshape(-1, count, head_dim)
        turned = rotate(heads_part, cosine_table, sine_table).reshape(array.shape[0], -1)
        return jnp.concatenate([turned, array[:, count * head_dim :]], axis=1).astype(BF16)

    rows_in = to_tokens([inputs[0]], n_rows, n_cols)
    packed = gather_cols(
        jnp.concatenate(
            [w_query, key_own, value_own, gain_attn[:, None], gain_ffn[:, None]], axis=1
        )
    )
    proj_w = packed[:, :proj_width]
    gain_one = packed[:, proj_width].astype(F32)
    gain_two = packed[:, proj_width + 1].astype(F32)
    out_w = gather_cols(w_out.T)
    gate_up_w = gather_cols(jnp.concatenate([w_gate, w_up], axis=1))
    down_w = gather_cols(w_down.T)
    kept = []
    results = []
    for m in range(batches):
        entered = rows_in[m] if m == 0 else after(rows_in[m], kept[-1][12])
        row_in = entered.astype(F32)
        inverse_one = lax.rsqrt(jnp.mean(row_in * row_in, axis=1, keepdims=True) + eps_norm)
        normed_one = row_in * inverse_one
        all_one = gather_rows((normed_one * gain_one[None, :]).astype(BF16))
        counts = lengths[m, 0]
        start = (in_order - slab_layout(counts, in_order))[:, None]
        cosine_table, sine_table = rope_tables(slab_layout(counts, places), head_dim)
        tables = (
            (cosine_table[:middle], cosine_table[middle:]),
            (sine_table[:middle], sine_table[middle:]),
        )
        turned = each(
            lambda side, cosine, sine: turn(dot_nn(side, proj_w), cosine, sine, heads + 1),
            all_one, *tables,
        )
        qkv = jnp.concatenate(turned, axis=0).reshape(wide)
        mixed, totals = attention_forward(rows, start, qkv, heads)
        mixed = halves(mixed)
        hidden_state = row_in + scatter_rows(mixed, out_w)
        inverse_two = lax.rsqrt(
            jnp.mean(hidden_state * hidden_state, axis=1, keepdims=True) + eps_norm
        )
        normed_two = hidden_state * inverse_two
        all_two = gather_rows((normed_two * gain_two[None, :]).astype(BF16))
        gate_both = each(lambda side: dot_nn(side, gate_up_w), all_two)

        def activate(both):
            gate_pre, upward = both[:, :ffn_width], both[:, ffn_width:]
            return (gate_pre * jax.nn.sigmoid(gate_pre) * upward).astype(BF16)

        hidden = each(activate, gate_both)
        gate_both = each(lambda both: both.astype(BF16), gate_both)
        result = hidden_state + scatter_rows(hidden, down_w)
        results.append(result.astype(BF16))
        if m == 0:
            rest = [inputs[n] for n in range(1, batches)]
            rest += [cotangent[n] for n in range(batches)]
            rest = to_tokens(rest, n_rows, n_cols, (mixed[0], down_w))
            rows_in += rest[: batches - 1]
            rows_dy = rest[batches - 1 :]
        kept.append(
            (
                all_one, normed_one, inverse_one, start, tables, qkv, mixed, totals,
                normed_two, inverse_two, all_two, gate_both, hidden,
            )
        )

    sums = {}
    grad_inputs = []
    for m in range(batches):
        (
            all_one, normed_one, inverse_one, start, tables, qkv, mixed, totals,
            normed_two, inverse_two, all_two, gate_both, hidden,
        ) = kept[m]
        begin = hidden if m == 0 else (hidden, grad_state)
        all_dy = gather_rows(after(rows_dy[m], begin))
        grad_down = outer(all_dy, hidden)

        def gate_backward(grad_hidden, both):
            gate_pre = both[:, :ffn_width].astype(F32)
            upward = both[:, ffn_width:].astype(F32)
            gate_sigma = jax.nn.sigmoid(gate_pre)
            grad_gate = grad_hidden * upward * gate_sigma * (1.0 + gate_pre * (1.0 - gate_sigma))
            grad_up = grad_hidden * gate_pre * gate_sigma
            return jnp.concatenate([grad_gate.astype(BF16), grad_up.astype(BF16)], axis=1)

        grad_hidden = each(lambda side: dot_nn(side, down_w), all_dy)
        grad_both = each(gate_backward, grad_hidden, gate_both)
        grad_gu = outer(all_two, grad_both)
        grad_two, gain_two_part = norm_backward(
            scatter_rows(grad_both, gate_up_w), normed_two, inverse_two, gain_two
        )
        grad_state = grad_two + rows_dy[m].astype(F32)
        final = m == batches - 1
        sums["down"] = grad_down if m == 0 else sums["down"] + grad_down
        sums["gu"] = grad_gu if m == 0 else sums["gu"] + grad_gu
        entering = grad_state.astype(BF16)
        if final:
            grad_down = scatter_cols(sums["down"])
            grad_gu = scatter_cols(sums["gu"])
            entering = gated(entering, grad_down)
        all_dh = gather_rows(entering)
        grad_out = outer(all_dh, mixed)
        sums["out"] = grad_out if m == 0 else sums["out"] + grad_out
        if final:
            grad_out = scatter_cols(sums["out"])
        grad_mixed = each(lambda side: dot_nn(side, out_w, BF16), all_dh)
        grad_mixed = jnp.concatenate(grad_mixed, axis=0).reshape(wide)
        if final:
            results = from_tokens(results, n_rows, n_cols)
            grad_mixed = gated(grad_mixed, results[0], grad_gu)
            early = from_tokens(grad_inputs, n_rows, n_cols)
        grad_qkv = halves(
            attention_backward(rows, start, qkv, totals, grad_mixed, heads)
        )
        grad_qkv = each(
            lambda side, cosine, sine: turn(side, cosine, -sine, heads + 1), grad_qkv, *tables
        )
        grad_proj = outer(all_one, grad_qkv)
        grad_one, gain_one_part = norm_backward(
            scatter_rows(grad_qkv, proj_w), normed_one, inverse_one, gain_one
        )
        grad_input = (grad_one + grad_state).astype(BF16)
        if final:
            grad_input = gated(grad_input, grad_out, early[0])
        grad_inputs.append(grad_input)
        terms = jnp.concatenate(
            [grad_proj, gain_one_part[:, None], gain_two_part[:, None]], axis=1
        )
        sums["proj"] = terms if m == 0 else sums["proj"] + terms

    late = from_tokens(grad_inputs[-1:], n_rows, n_cols)
    grad_inputs = [a.astype(F32) for a in early + late]
    grad_proj = scatter_cols(sums["proj"])
    shared = lax.all_gather(
        grad_proj[:, query_width:].astype(BF16), "rows", axis=0
    ).astype(F32)
    copies = shared.reshape(KEY_VALUE_HEADS, n_rows // KEY_VALUE_HEADS, *shared.shape[1:])
    heads_sum = jnp.sum(copies, axis=1)
    key_sum = jnp.transpose(heads_sum[:, :, :head_dim], (1, 0, 2)).reshape(key_weight.shape)
    value_sum = jnp.transpose(heads_sum[:, :, head_dim : 2 * head_dim], (1, 0, 2)).reshape(
        value_weight.shape
    )
    gains = jnp.sum(heads_sum[:, :, 2 * head_dim :], axis=0)
    return (
        jnp.stack(results),
        jnp.stack(grad_inputs),
        gains[:, 0],
        grad_proj[:, :query_width],
        key_sum,
        value_sum,
        grad_out.T,
        gains[:, 1],
        grad_gu[:, :ffn_width],
        grad_gu[:, ffn_width:],
        grad_down.T,
    )


def solution(mesh):
    in_specs = (
        P(None, "rows", "cols"),
        P(None, "cols", None),
        P("cols"),
        P("cols", "rows"),
        P("cols", None),
        P("cols", None),
        P("rows", "cols"),
        P("cols"),
        P("cols", "rows"),
        P("cols", "rows"),
        P("rows", "cols"),
        P(None, "rows", "cols"),
    )
    out_specs = (
        P(None, "rows", "cols"),
        P(None, "rows", "cols"),
        P("cols"),
        P("cols", "rows"),
        P("cols", None),
        P("cols", None),
        P("rows", "cols"),
        P("cols"),
        P("cols", "rows"),
        P("cols", "rows"),
        P("rows", "cols"),
    )
    return jax.shard_map(local, mesh=mesh, in_specs=in_specs, out_specs=out_specs, check_vma=False)
```
